32 devices in a mesh: seq: 8 (over z, y), head: 4 (over x, core).
Axes of the slice: x: 2, y: 2, z: 4, core: 2. Of those that a mesh axis runs over, the one named last changes fastest.
Arguments:
- seq_inputs: bfloat16 [1, 2048, 4096], P(None, 'seq', 'head'), may hold values from -6 to 6
- gate_inputs: bfloat16 [1, 2048, 4096], P(None, 'seq', 'head'), may hold values from -6 to 6
- projections: bfloat16 [1, 2048, 256], P(None, 'seq'), may hold values from -6 to 6
- step_raw: float32 [1, 2048, 64], P(None, 'seq', 'head'), may hold values from -3 to 3
- step_bias: float32 [64], P('head'), may hold values from -1 to 1
- decay_rate: float32 [64], P('head'), may hold values from 0.00048828125 to 8
- conv_feature: float32 [4, 4096], P(None, 'head'), may hold values from -3 to 3
- conv_proj: float32 [4, 256], replicated, may hold values from -3 to 3
- norm_gain: float32 [4096], P('head'), may hold values from 0.25 to 1.75
Outputs:
- mixed_out: bfloat16 [1, 2048, 4096], P(None, 'seq', 'head')
The draws below stay inside these ranges and needn't reach their ends.
All inputs are finite; a program needn't handle non-finite values.
Results may differ from the reference program's by a relative error of at most 0.0034.
Values may be sent and summed in bfloat16 or wider, within the bound.
A program may use at most 192 MiB of HBM per device.

```python
import math
import jax
import jax.numpy as jnp
from jax import lax

HEADS = 64
HEAD_DIM = 64
STATE = 128
CONV = 4
STRETCH = 256
BATCH = 1
TOKENS = 2048


def block_scale(own_key, shape, pieces, low, largest):
    def one(position, parts):
        draws = jax.random.uniform(jax.random.fold_in(jax.random.fold_in(own_key, 6), position), (parts,), jnp.float32, low / len(pieces), largest / len(pieces))
        return jnp.repeat(jnp.exp(draws), shape[position] // parts).reshape((-1,) + (1,) * (len(shape) - position - 1))

    gain = one(*pieces[0])
    for cut in pieces[1:]:
        gain = gain * one(*cut)
    return gain


def centred(stream_key, shape, width, limit, split=(), kind=jnp.bfloat16):
    result = width * jax.random.normal(stream_key, shape, jnp.float32)
    if split:
        result = result * block_scale(stream_key, shape, split, -0.22, 0.18)
    return jnp.clip(result, -limit, limit).astype(kind)


def setup_inputs(seed: int = 0) -> dict:
    streams_of = jax.random.split(jax.random.key(seed), 10)
    return {
        "seq_inputs": centred(streams_of[0], (BATCH, TOKENS, HEADS * HEAD_DIM), 1.0, 6.0, ((1, 8), (2, 4))),
        "gate_inputs": centred(streams_of[1], (BATCH, TOKENS, HEADS * HEAD_DIM), 1.0, 6.0, ((1, 8), (2, 4))),
        "projections": centred(streams_of[2], (BATCH, TOKENS, 2 * STATE), 1.0, 6.0, ((1, 8),)),
        "step_raw": centred(streams_of[3], (BATCH, TOKENS, HEADS), 0.5, 3.0, ((1, 8), (2, 4)), jnp.float32),
        "step_bias": jnp.clip(jax.random.uniform(streams_of[4], (HEADS,), jnp.float32, -1.0, 1.0) * block_scale(streams_of[4], (HEADS,), ((0, 4),), -0.4, 0.0), -1.0, 1.0),
        "decay_rate": jnp.clip(jnp.exp(math.log(8.0) - 9.704061 * jax.random.uniform(streams_of[5], (HEADS,), jnp.float32) ** block_scale(streams_of[5], (HEADS,), ((0, 4),), -0.2, 0.2)), 0.00048828125, 8.0),
        "conv_feature": centred(streams_of[6], (CONV, HEADS * HEAD_DIM), CONV ** -0.5, 3.0, ((1, 4),), jnp.float32),
        "conv_proj": centred(streams_of[7], (CONV, 2 * STATE), CONV ** -0.5, 3.0, (), jnp.float32),
        "norm_gain": jnp.clip(1.0 + 0.15 * jax.random.normal(streams_of[8], (HEADS * HEAD_DIM,), jnp.float32), 0.25, 1.75),
    }


def settle(values):
    return lax.optimization_barrier(values.astype(jnp.bfloat16)).astype(jnp.float32)

def causal_mix(window, weights):
    kernel_len = weights.shape[0]
    length = window.shape[1] - kernel_len + 1
    running = window[:, 0:length].astype(jnp.float32) * weights[0]
    for offset in range(1, kernel_len):
        running = running + window[:, offset:offset + length].astype(jnp.float32) * weights[offset]
    return settle(jax.nn.silu(running))

def block_terms(x_mixed, write_vec, read_vec, step_size, decay_rate, carried):
    log_decay = jnp.cumsum(step_size * -decay_rate, axis=1)
    scores = jnp.einsum('btn,bsn->bts', read_vec, write_vec)
    causal = jnp.arange(STRETCH)[:, None] >= jnp.arange(STRETCH)[None, :]
    decay_gap = jnp.where(causal[None, :, :, None], log_decay[:, :, None, :] - log_decay[:, None, :, :], 0.0)
    mixing = settle(jnp.where(causal[None, :, :, None], scores[:, :, :, None] * jnp.exp(decay_gap) * step_size[:, None, :, :], 0.0))
    within = jnp.einsum('btsh,bshp->bthp', mixing, x_mixed)
    to_end = jnp.exp(log_decay[:, -1:, :] - log_decay) * step_size
    weighted = settle(x_mixed * to_end[:, :, :, None])
    summary = jnp.einsum('bshp,bsn->bhpn', weighted, write_vec)
    outside = jnp.einsum('bhpn,btn->bthp', settle(carried), read_vec) * jnp.exp(log_decay)[:, :, :, None]
    next_carried = jnp.exp(log_decay[:, -1, :])[:, :, None, None] * carried + summary
    return (within + outside, next_carried)

def reference(seq_inputs, gate_inputs, projections, step_raw, step_bias, decay_rate, conv_feature, conv_proj, norm_gain):
    kernel_len = conv_feature.shape[0]
    padded_x = jnp.pad(seq_inputs, ((0, 0), (kernel_len - 1, 0), (0, 0)))
    padded_proj = jnp.pad(projections, ((0, 0), (kernel_len - 1, 0), (0, 0)))

    def advance(carried, block_id):
        start = (block_id * STRETCH).astype(jnp.int32)
        window_x = lax.dynamic_slice_in_dim(padded_x, start, STRETCH + kernel_len - 1, 1)
        window_proj = lax.dynamic_slice_in_dim(padded_proj, start, STRETCH + kernel_len - 1, 1)
        x_mixed = causal_mix(window_x, conv_feature).reshape(BATCH, STRETCH, HEADS, HEAD_DIM)
        proj_mixed = causal_mix(window_proj, conv_proj)
        write_vec = proj_mixed[:, :, :STATE]
        read_vec = proj_mixed[:, :, STATE:]
        step_size = jax.nn.softplus(lax.dynamic_slice_in_dim(step_raw, start, STRETCH, 1) + step_bias)
        outputs, carried = block_terms(x_mixed, write_vec, read_vec, step_size, decay_rate, carried)
        gate_block = lax.dynamic_slice_in_dim(gate_inputs, start, STRETCH, 1)
        gated = outputs.reshape(BATCH, STRETCH, HEADS * HEAD_DIM) * jax.nn.silu(gate_block.astype(jnp.float32))
        scale = lax.rsqrt(lax.optimization_barrier(jnp.mean(gated * gated, axis=-1)) + 1.0)
        return (carried, (gated * scale[:, :, None] * norm_gain).astype(jnp.bfloat16))
    initial = jnp.zeros((BATCH, HEADS, HEAD_DIM, STATE), jnp.float32)
    _, stacked = lax.scan(advance, initial, jnp.arange(TOKENS // STRETCH, dtype=jnp.int32))
    return jnp.transpose(stacked, (1, 0, 2, 3)).reshape(BATCH, TOKENS, HEADS * HEAD_DIM)
```

```python
import functools
import math

import jax
import jax.numpy as jnp
from jax import lax
from jax.experimental import pallas as pl
from jax.experimental.pallas import tpu as pltpu
from jax.sharding import PartitionSpec as P

HEADS = 64
HEAD_DIM = 64
STRETCH = 256
LANES = 128
LOG2E = math.log2(math.e)
MESH = pl.DeviceIdType.MESH


def silu(value):
    half = 0.5 * value
    return half + half * jnp.tanh(half)


def pieces(value, count):
    parts = []
    for _ in range(count):
        part = value.astype(jnp.bfloat16)
        parts.append(part)
        value = value - part.astype(jnp.float32)
    return parts


def dot(a, b):
    return jnp.dot(a, b, preferred_element_type=jnp.float32)


def dot_parts(parts, b):
    total = dot(parts[-1], b)
    for part in parts[-2::-1]:
        total = total + dot(part, b)
    return total


def iota(shape, dim):
    return lax.broadcasted_iota(jnp.int32, shape, dim)


def conv(wide, slot, halo, rows, weights):
    span = rows.shape[0]
    taps = weights.shape[0]
    wide[slot, 0:8] = halo.astype(jnp.float32)
    wide[slot, 8 : 8 + span] = rows.astype(jnp.float32)
    first = 8 - taps + 1
    total = wide[slot, first : first + span] * weights[0:1]
    for k in range(1, taps):
        total = total + wide[slot, first + k : first + k + span] * weights[k : k + 1]
    return silu(total)


def kernel(
    n,
    m,
    total_channels,
    x_hbm,
    gate_hbm,
    proj_hbm,
    raw_hbm,
    bias_ref,
    rate_ref,
    cf_ref,
    cp_ref,
    gain_ref,
    out_ref,
    x_v,
    gate_v,
    proj_v,
    raw_v,
    halo_x,
    halo_p,
    wide_x,
    wide_p,
    pad,
    m_t,
    xm,
    within,
    s_send,
    s_recv,
    s_own,
    d_own,
    d_recv,
    p_in,
    p_out,
    e_own,
    e_send,
    e_recv,
    sq_send,
    sq_recv,
    x_sem,
    gate_sem,
    misc_sem,
    halo_s,
    halo_r,
    d_s,
    d_r,
    s_s,
    s_r,
    p_s,
    p_r,
    e_s,
    e_r,
    sq_s,
    sq_r,
):
    span = proj_v.shape[1]
    chunks = x_v.shape[0]
    half = chunks // 2
    heads = rate_ref.shape[1]
    per = heads // chunks
    width = LANES // per
    i = lax.axis_index("seq")
    hd = lax.axis_index("head")
    y = lax.rem(i, 2)
    partner = i + 1 - 2 * y
    has_prev, has_next = i > 0, i < n - 1
    has_before, has_after = i >= 2, i < n - 2

    barrier = pltpu.get_barrier_semaphore()
    relations = [(has_prev, i - 1), (has_next, i + 1), (has_before, i - 2), (has_after, i + 2)]
    for here, who in relations:

        @pl.when(here)
        def _():
            pl.semaphore_signal(barrier, inc=1, device_id=(who, hd), device_id_type=MESH)

    for k in range(1, m):
        pl.semaphore_signal(
            barrier, inc=1, device_id=(i, lax.rem(hd + k, m)), device_id_type=MESH
        )

    raw_copy = pltpu.make_async_copy(raw_hbm, raw_v, misc_sem.at[0])
    raw_copy.start()
    proj_copies = [
        pltpu.make_async_copy(
            proj_hbm.at[:, k * LANES : (k + 1) * LANES], proj_v.at[k], misc_sem.at[1 + k]
        )
        for k in range(2)
    ]
    for copy in proj_copies:
        copy.start()
    x_copies = []
    gate_copies = []
    for c in range(chunks):
        cols = slice(c * LANES, (c + 1) * LANES)
        x_copies.append(pltpu.make_async_copy(x_hbm.at[:, cols], x_v.at[c], x_sem.at[c]))
        gate_copies.append(
            pltpu.make_async_copy(gate_hbm.at[:, cols], gate_v.at[c], gate_sem.at[c])
        )
    for copy in x_copies + gate_copies:
        copy.start()

    pl.semaphore_wait(barrier, sum(here.astype(jnp.int32) for here, _ in relations) + m - 1)

    halo_rows = halo_x.shape[0]
    halos = [
        pltpu.make_async_remote_copy(
            src_ref=src.at[span - halo_rows : span],
            dst_ref=dst,
            send_sem=halo_s.at[k],
            recv_sem=halo_r.at[k],
            device_id=(lax.rem(i + 1, n), hd),
            device_id_type=MESH,
        )
        for k, (src, dst) in enumerate([(x_hbm, halo_x), (proj_hbm, halo_p)])
    ]

    @pl.when(has_next)
    def _():
        for copy in halos:
            copy.start()

    raw_copy.wait()
    shifted = raw_v[...] + bias_ref[...]
    step = jnp.maximum(shifted, 0.0) + jnp.log1p(jnp.exp(-jnp.abs(shifted)))
    tri = (iota((span, span), 0) >= iota((span, span), 1)).astype(jnp.bfloat16)
    lead = (step * (-LOG2E)) * rate_ref[...]
    run = None
    for part in reversed(pieces(lead, 3)):
        term = dot(tri, part)
        run = term if run is None else run + term
    source = run - LOG2E * jnp.log(step)
    last = run[span - 1 : span]
    to_end = pieces(jnp.exp2(last - source), 2)
    decay_now = pieces(jnp.exp2(run), 2)
    pad[...] = jnp.zeros_like(pad)
    pad[:, 0:heads] = source
    m_t[...] = jnp.transpose(pad[...])

    def spread(parts, c):
        pick = iota((heads, LANES), 0) == c * per + iota((heads, LANES), 1) // width
        return dot_parts(parts, pick.astype(jnp.bfloat16))

    owner = iota((chunks, heads), 1) // per == iota((chunks, heads), 0)
    ends = jnp.where(owner, jnp.broadcast_to(jnp.exp2(last), (chunks, heads)), 0.0)
    lane_of = iota((heads, LANES), 0) % per == iota((heads, LANES), 1) // width
    d_own[...] = dot_parts(pieces(ends, 3), lane_of.astype(jnp.bfloat16))

    def to_partner(src, dst, send_sem, recv_sem):
        return pltpu.make_async_remote_copy(
            src_ref=src,
            dst_ref=dst,
            send_sem=send_sem,
            recv_sem=recv_sem,
            device_id=(partner, hd),
            device_id_type=MESH,
        )

    d_copy = to_partner(d_own, d_recv, d_s, d_r)
    d_copy.start()

    for copy in proj_copies + x_copies:
        copy.wait()

    @pl.when(has_prev)
    def _():
        for copy in halos:
            copy.wait_recv()

    @pl.when(i == 0)
    def _():
        halo_x[...] = jnp.zeros_like(halo_x)
        halo_p[...] = jnp.zeros_like(halo_p)

    mixed = []
    for k in range(2):
        cols = slice(k * LANES, (k + 1) * LANES)
        mixed.append(
            conv(wide_p, k, halo_p[halo_rows - 8 :, cols], proj_v[k], cp_ref[:, cols])
        )
    write_t = jnp.transpose(mixed[0]).astype(jnp.bfloat16)
    read_vec = mixed[1].astype(jnp.bfloat16)

    def summarize(c):
        cols = pl.ds(pl.multiple_of(c * LANES, LANES), LANES)
        x_c = conv(wide_x, c, halo_x[halo_rows - 8 :, cols], x_v[c], cf_ref[:, cols])
        x_c = x_c.astype(jnp.bfloat16)
        xm[c] = x_c
        weighted = (x_c.astype(jnp.float32) * spread(to_end, c)).astype(jnp.bfloat16)
        return dot(write_t, weighted)

    s_copies = [
        to_partner(s_send.at[j], s_recv.at[j], s_s.at[j], s_r.at[j]) for j in range(half)
    ]
    for j in range(half):
        s_send[j] = summarize((1 - y) * half + j).astype(jnp.bfloat16)
        s_copies[j].start()
    for j in range(half):
        s_own[j] = summarize(y * half + j)

    scores = dot(read_vec, write_t)
    side = LANES
    steps_in = span // side
    causal = iota((side, side), 0) >= iota((side, side), 1)
    low = iota((span, LANES), 1) // width

    def inside(c):
        x_c = xm[c]
        totals = [None] * steps_in
        for q in range(per):
            h = c * per + q
            x_q = jnp.where(low == q, x_c.astype(jnp.float32), 0.0).astype(jnp.bfloat16)
            for r in range(steps_in):
                rows = slice(r * side, (r + 1) * side)
                now = run[rows, h : h + 1]
                tiles = []
                for k in range(r + 1):
                    cols = slice(k * side, (k + 1) * side)
                    gap = now - m_t[h : h + 1, cols]
                    if k == r:
                        gap = jnp.where(causal, gap, -1e30)
                    tiles.append((scores[rows, cols] * jnp.exp2(gap)).astype(jnp.bfloat16))
                mixing = tiles[0] if r == 0 else jnp.concatenate(tiles, axis=1)
                term = dot(mixing, x_q[0 : (r + 1) * side])
                totals[r] = term if totals[r] is None else totals[r] + term
        for r in range(steps_in):
            within[c, r * side : (r + 1) * side] = totals[r]

    @pl.when(i < 2)
    def _():
        p_in[...] = jnp.zeros_like(p_in)

    p_copies = [
        pltpu.make_async_remote_copy(
            src_ref=p_out.at[j],
            dst_ref=p_in.at[j],
            send_sem=p_s.at[j],
            recv_sem=p_r.at[j],
            device_id=(lax.rem(i + 2, n), hd),
            device_id_type=MESH,
        )
        for j in range(half)
    ]
    e_copies = [
        to_partner(e_send.at[j], e_recv.at[j], e_s.at[j], e_r.at[j]) for j in range(half)
    ]

    early = y == 0
    d_copy.wait_recv()
    queue = list(range(chunks))
    for _ in range(2):
        inside(queue.pop(0))
    for j in range(half):
        s_copies[j].wait_recv()

        @pl.when(has_before)
        def _():
            p_copies[j].wait_recv()

        c = y * half + j
        d_mine = d_own[pl.ds(c, 1), :]
        d_other = d_recv[pl.ds(c, 1), :]
        d_first = jnp.where(early, d_mine, d_other)
        d_second = jnp.where(early, d_other, d_mine)
        mine = s_own[j]
        other = s_recv[j].astype(jnp.float32)
        first = jnp.where(early, mine, other)
        second = jnp.where(early, other, mine)
        before = p_in[j].astype(jnp.float32)
        middle = d_first * before + first

        @pl.when(has_after)
        def _():
            p_out[j] = (d_second * middle + second).astype(jnp.bfloat16)
            p_copies[j].start()

        e_own[j] = jnp.where(early, before, middle).astype(jnp.bfloat16)
        e_send[j] = jnp.where(early, middle, before).astype(jnp.bfloat16)
        e_copies[j].start()
        if queue:
            inside(queue.pop(0))
    while queue:
        inside(queue.pop(0))

    for copy in gate_copies:
        copy.wait()
    squares = jnp.zeros((span, LANES), jnp.float32)

    def gate(c, state, squares):
        outside = dot(read_vec, state) * spread(decay_now, c)
        gated = (within[c] + outside) * silu(gate_v[c].astype(jnp.float32))
        within[c] = gated
        return squares + gated * gated

    for j in range(half):
        squares = gate(y * half + j, e_own[j], squares)
    for j in range(half):
        e_copies[j].wait_recv()
        squares = gate((1 - y) * half + j, e_recv[j], squares)

    row = jnp.sum(jnp.transpose(squares), axis=0, keepdims=True)
    sq_send[...] = jnp.broadcast_to(row, sq_send.shape)
    sq_copies = [
        pltpu.make_async_remote_copy(
            src_ref=sq_send,
            dst_ref=sq_recv.at[k - 1],
            send_sem=sq_s.at[k - 1],
            recv_sem=sq_r.at[k - 1],
            device_id=(i, lax.rem(hd + k, m)),
            device_id_type=MESH,
        )
        for k in range(1, m)
    ]
    for copy in sq_copies:
        copy.start()
    for copy in sq_copies:
        copy.wait_recv()
    for k in range(1, m):
        row = row + sq_recv[k - 1, 0:1]
    scale = lax.rsqrt(row / total_channels + 1.0)
    scale = jnp.transpose(jnp.broadcast_to(scale, (LANES, span)))
    for c in range(chunks):
        cols = slice(c * LANES, (c + 1) * LANES)
        out_ref[:, cols] = (within[c] * scale * gain_ref[:, cols]).astype(jnp.bfloat16)

    @pl.when(has_next)
    def _():
        for copy in halos:
            copy.wait_send()

    d_copy.wait_send()
    for copy in s_copies + e_copies + sq_copies:
        copy.wait_send()

    @pl.when(has_after)
    def _():
        for copy in p_copies:
            copy.wait_send()


def shards(n, m, x, gate, proj, raw, bias, rate, cf, cp, gain):
    _, span, channels = x.shape
    heads = rate.shape[0]
    chunks = channels // LANES
    half = chunks // 2
    state = proj.shape[2] // 2
    f32, bf16 = jnp.float32, jnp.bfloat16
    dma = pltpu.SemaphoreType.DMA
    any_spec = pl.BlockSpec(memory_space=pl.ANY)
    vmem = pl.BlockSpec(memory_space=pltpu.VMEM)
    result = pl.pallas_call(
        functools.partial(kernel, n, m, channels * m),
        out_shape=jax.ShapeDtypeStruct((span, channels), bf16),
        in_specs=[any_spec] * 4 + [vmem] * 5,
        out_specs=vmem,
        scratch_shapes=[
            pltpu.VMEM((chunks, span, LANES), bf16),
            pltpu.VMEM((chunks, span, LANES), bf16),
            pltpu.VMEM((2, span, LANES), bf16),
            pltpu.VMEM((span, heads), f32),
            pltpu.VMEM((16, channels), bf16),
            pltpu.VMEM((16, 2 * state), bf16),
            pltpu.VMEM((chunks, span + 8, LANES), f32),
            pltpu.VMEM((2, span + 8, LANES), f32),
            pltpu.VMEM((span, LANES), f32),
            pltpu.VMEM((LANES, span), f32),
            pltpu.VMEM((chunks, span, LANES), bf16),
            pltpu.VMEM((chunks, span, LANES), f32),
            pltpu.VMEM((half, state, LANES), bf16),
            pltpu.VMEM((half, state, LANES), bf16),
            pltpu.VMEM((half, state, LANES), f32),
            pltpu.VMEM((chunks, LANES), f32),
            pltpu.VMEM((chunks, LANES), f32),
            pltpu.VMEM((half, state, LANES), bf16),
            pltpu.VMEM((half, state, LANES), bf16),
            pltpu.VMEM((half, state, LANES), bf16),
            pltpu.VMEM((half, state, LANES), bf16),
            pltpu.VMEM((half, state, LANES), bf16),
            pltpu.VMEM((8, span), f32),
            pltpu.VMEM((m - 1, 8, span), f32),
            dma((chunks,)),
            dma((chunks,)),
            dma((3,)),
            dma((2,)),
            dma((2,)),
            dma,
            dma,
            dma((half,)),
            dma((half,)),
            dma((half,)),
            dma((half,)),
            dma((half,)),
            dma((half,)),
            dma((m - 1,)),
            dma((m - 1,)),
        ],
        compiler_params=pltpu.CompilerParams(collective_id=0, has_side_effects=True),
    )(x[0], gate[0], proj[0], raw[0], bias[None], rate[None], cf, cp, gain[None])
    return result[None]


def solution(mesh):
    sizes = mesh.shape
    return jax.shard_map(
        functools.partial(shards, sizes["seq"], sizes["head"]),
        mesh=mesh,
        in_specs=(
            P(None, "seq", "head"),
            P(None, "seq", "head"),
            P(None, "seq", None),
            P(None, "seq", "head"),
            P("head"),
            P("head"),
            P(None, "head"),
            P(),
            P("head"),
        ),
        out_specs=P(None, "seq", "head"),
        check_vma=False,
    )
```

```python
import functools
import math

import jax
import jax.numpy as jnp
from jax import lax
from jax.experimental import pallas as pl
from jax.experimental.pallas import tpu as pltpu
from jax.sharding import PartitionSpec as P

HEADS = 64
HEAD_DIM = 64
STRETCH = 256
LANES = 128
LOG2E = math.log2(math.e)
FIX = 16
SPLIT = 2
BEFORE = 4
MESH = pl.DeviceIdType.MESH


def silu(value):
    half = 0.5 * value
    return half + half * jnp.tanh(half)


def pieces(value, count):
    parts = []
    for _ in range(count):
        part = value.astype(jnp.bfloat16)
        parts.append(part)
        value = value - part.astype(jnp.float32)
    return parts


def dot(a, b):
    return jnp.dot(a, b, preferred_element_type=jnp.float32)


def dot_parts(parts, b):
    total = dot(parts[-1], b)
    for part in parts[-2::-1]:
        total = total + dot(part, b)
    return total


def iota(shape, dim):
    return lax.broadcasted_iota(jnp.int32, shape, dim)


def conv(wide, slot, weights, span):
    taps = weights.shape[0]
    first = 8 - taps + 1
    total = wide[slot, first : first + span] * weights[0:1]
    for k in range(1, taps):
        total = total + wide[slot, first + k : first + k + span] * weights[k : k + 1]
    return silu(total)


def kernel(
    n,
    m,
    total_channels,
    x_hbm,
    gate_hbm,
    proj_hbm,
    raw_hbm,
    bias_ref,
    rate_ref,
    cf_ref,
    cp_ref,
    gain_ref,
    out_ref,
    x_v,
    gate_v,
    proj_v,
    raw_v,
    halo_out,
    halo_in,
    wide_x,
    wide_p,
    xm,
    within,
    factor,
    s_part,
    out_v,
    s_send,
    s_recv,
    s_own,
    d_own,
    d_recv,
    p_in,
    p_out,
    e_own,
    e_send,
    e_recv,
    sq_send,
    sq_recv,
    x_sem,
    gate_sem,
    misc_sem,
    out_sem,
    halo_s,
    halo_r,
    d_s,
    d_r,
    s_s,
    s_r,
    p_s,
    p_r,
    e_s,
    e_r,
    sq_s,
    sq_r,
):
    span = proj_v.shape[1]
    chunks = x_v.shape[0]
    half = chunks // 2
    heads = rate_ref.shape[1]
    per = heads // chunks
    width = LANES // per
    i = lax.axis_index("seq")
    hd = lax.axis_index("head")
    y = lax.rem(i, 2)
    partner = i + 1 - 2 * y
    has_prev, has_next = i > 0, i < n - 1
    has_before, has_after = i >= 2, i < n - 2

    barrier = pltpu.get_barrier_semaphore()
    relations = [(has_prev, i - 1), (has_next, i + 1), (has_before, i - 2), (has_after, i + 2)]
    for here, who in relations:

        @pl.when(here)
        def _():
            pl.semaphore_signal(barrier, inc=1, device_id=(who, hd), device_id_type=MESH)

    for k in range(1, m):
        pl.semaphore_signal(
            barrier, inc=1, device_id=(i, lax.rem(hd + k, m)), device_id_type=MESH
        )

    channels = chunks * LANES
    edge = span - halo_in.shape[0]
    edge_copies = [
        pltpu.make_async_copy(
            x_hbm.at[edge:span], halo_out.at[:, 0:channels], misc_sem.at[3]
        ),
        pltpu.make_async_copy(
            proj_hbm.at[edge:span], halo_out.at[:, channels:], misc_sem.at[4]
        ),
    ]
    raw_copy = pltpu.make_async_copy(raw_hbm, raw_v, misc_sem.at[0])
    proj_copies = [
        pltpu.make_async_copy(
            proj_hbm.at[:, k * LANES : (k + 1) * LANES], proj_v.at[k], misc_sem.at[1 + k]
        )
        for k in range(2)
    ]
    for copy in edge_copies + [raw_copy] + proj_copies:
        copy.start()
    x_copies = []
    gate_copies = []
    for c in range(chunks):
        cols = slice(c * LANES, (c + 1) * LANES)
        x_copies.append(pltpu.make_async_copy(x_hbm.at[:, cols], x_v.at[c], x_sem.at[c]))
        gate_copies.append(
            pltpu.make_async_copy(gate_hbm.at[:, cols], gate_v.at[c], gate_sem.at[c])
        )
    for copy in x_copies + gate_copies:
        copy.start()
    for copy in edge_copies:
        copy.wait()

    pl.semaphore_wait(barrier, sum(here.astype(jnp.int32) for here, _ in relations) + m - 1)

    halo_copy = pltpu.make_async_remote_copy(
        src_ref=halo_out,
        dst_ref=halo_in,
        send_sem=halo_s,
        recv_sem=halo_r,
        device_id=(lax.rem(i + 1, n), hd),
        device_id_type=MESH,
    )

    @pl.when(has_next)
    def _():
        halo_copy.start()

    def column(row):
        eye = iota((heads, heads), 0) == iota((heads, heads), 1)
        wide = jnp.broadcast_to(row, (heads, heads))
        return jnp.sum(jnp.where(eye, wide, 0.0), axis=1, keepdims=True)

    raw_copy.wait()
    shifted = raw_v[...] + column(bias_ref[...])
    step = jnp.maximum(shifted, 0.0) + jnp.log1p(jnp.exp(-jnp.abs(shifted)))
    upto = (iota((span, span), 0) <= iota((span, span), 1)).astype(jnp.bfloat16)
    lead = (step * (-LOG2E)) * column(rate_ref[...])
    run_t = dot_parts(pieces(lead, 3), upto)
    source_t = run_t - LOG2E * jnp.log(step)
    last = run_t[:, span - 1 : span]
    to_end = jnp.exp2(last - source_t)
    token = iota((heads, span), 1)
    rows = [
        run_t,
        jnp.where(token < FIX, 0.0, to_end),
        jnp.exp2(run_t),
        jnp.where(token < FIX, to_end, 0.0),
    ]
    rows.append(jnp.zeros((LANES - len(rows) * heads, span), jnp.float32))
    table = jnp.transpose(jnp.concatenate(rows, axis=0))
    run = table
    table_parts = pieces(jnp.where(iota((span, LANES), 1) < heads, 0.0, table), 2)
    fix_parts = [part[0:FIX] for part in table_parts]

    def spread(parts, kind, c):
        source = kind * heads + c * per + iota((LANES, LANES), 1) // width
        return dot_parts(parts, (iota((LANES, LANES), 0) == source).astype(jnp.bfloat16))

    lane_of = iota((heads, LANES), 0) % per == iota((heads, LANES), 1) // width
    ends = jnp.where(lane_of, jnp.exp2(last), 0.0)
    owner = (iota((chunks, heads), 1) // per == iota((chunks, heads), 0)).astype(jnp.bfloat16)
    ends_parts = pieces(ends, 3)
    d_own[...] = dot(owner, ends_parts[2]) + dot(owner, ends_parts[1]) + dot(owner, ends_parts[0])

    def to_partner(src, dst, send_sem, recv_sem):
        return pltpu.make_async_remote_copy(
            src_ref=src,
            dst_ref=dst,
            send_sem=send_sem,
            recv_sem=recv_sem,
            device_id=(partner, hd),
            device_id_type=MESH,
        )

    d_copy = to_partner(d_own, d_recv, d_s, d_r)
    d_copy.start()

    for copy in proj_copies:
        copy.wait()
    mixed = []
    for k in range(2):
        cols = slice(k * LANES, (k + 1) * LANES)
        wide_p[k, 0:8] = jnp.zeros((8, LANES), jnp.float32)
        wide_p[k, 8 : 8 + span] = proj_v[k].astype(jnp.float32)
        mixed.append(conv(wide_p, k, cp_ref[:, cols], span))
    write_t = jnp.transpose(mixed[0])
    write_main = write_t.astype(jnp.bfloat16)

    for c in range(chunks):
        x_copies[c].wait()
        wide_x[c, 0:8] = jnp.zeros((8, LANES), jnp.float32)
        wide_x[c, 8 : 8 + span] = x_v[c].astype(jnp.float32)
        x_c = conv(wide_x, c, cf_ref[:, c * LANES : (c + 1) * LANES], span)
        x_c = x_c.astype(jnp.bfloat16)
        xm[c] = x_c
        weighted = x_c.astype(jnp.float32) * spread(table_parts, 1, c)
        s_part[c] = dot(write_main, weighted.astype(jnp.bfloat16))

    @pl.when(has_prev)
    def _():
        halo_copy.wait_recv()

    @pl.when(i == 0)
    def _():
        halo_in[...] = jnp.zeros_like(halo_in)

    fixed = []
    for k in range(2):
        cols = slice(k * LANES, (k + 1) * LANES)
        lanes = slice(channels + k * LANES, channels + (k + 1) * LANES)
        wide_p[k, 0:8] = halo_in[:, lanes].astype(jnp.float32)
        fixed.append(conv(wide_p, k, cp_ref[:, cols], FIX))
    blank = jnp.zeros((LANES - FIX, LANES), jnp.float32)
    fix_t = jnp.transpose(jnp.concatenate([fixed[0], blank], axis=0))
    fix_write = fix_t[:, 0:FIX].astype(jnp.bfloat16)

    def summarize(c):
        cols = pl.ds(pl.multiple_of(c * LANES, LANES), LANES)
        wide_x[c, 0:8] = halo_in[:, cols].astype(jnp.float32)
        x_c = conv(wide_x, c, cf_ref[:, cols], FIX).astype(jnp.bfloat16)
        xm[c, 0:FIX] = x_c
        weighted = x_c.astype(jnp.float32) * spread(fix_parts, 3, c)
        return s_part[c] + dot(fix_write, weighted.astype(jnp.bfloat16))

    count = half * SPLIT
    tall = s_own.shape[1] // SPLIT
    s_copies = [
        to_partner(s_send.at[j], s_recv.at[j], s_s.at[j], s_r.at[j]) for j in range(count)
    ]
    for j in range(half):
        sent = summarize((1 - y) * half + j).astype(jnp.bfloat16)
        for r in range(SPLIT):
            s_send[j * SPLIT + r] = sent[r * tall : (r + 1) * tall]
            s_copies[j * SPLIT + r].start()
    for j in range(half):
        s_own[j] = summarize(y * half + j)

    head_t = jnp.where(iota((LANES, LANES), 1) < FIX, fix_t, write_t[:, 0:LANES])
    write_t = jnp.concatenate([head_t, write_t[:, LANES:]], axis=1).astype(jnp.bfloat16)
    read_vec = jnp.concatenate([fixed[1], mixed[1][FIX:]], axis=0).astype(jnp.bfloat16)
    scores = dot(read_vec, write_t)
    side = LANES
    steps_in = span // side
    causal = iota((side, side), 0) >= iota((side, side), 1)
    low = iota((span, LANES), 1) // width

    def inside(c):
        x_c = xm[c]
        totals = [None] * steps_in
        for q in range(per):
            h = c * per + q
            x_q = jnp.where(low == q, x_c.astype(jnp.float32), 0.0).astype(jnp.bfloat16)
            for r in range(steps_in):
                rows = slice(r * side, (r + 1) * side)
                now = run[rows, h : h + 1]
                tiles = []
                for k in range(r + 1):
                    cols = slice(k * side, (k + 1) * side)
                    gap = now - source_t[h : h + 1, cols]
                    if k == r:
                        gap = jnp.where(causal, gap, -1e30)
                    tiles.append((scores[rows, cols] * jnp.exp2(gap)).astype(jnp.bfloat16))
                mixing = tiles[0] if r == 0 else jnp.concatenate(tiles, axis=1)
                term = dot(mixing, x_q[0 : (r + 1) * side])
                totals[r] = term if totals[r] is None else totals[r] + term
        gate_copies[c].wait()
        for r in range(steps_in):
            rows = slice(r * side, (r + 1) * side)
            gate = silu(gate_v[c, rows].astype(jnp.float32))
            within[c, rows] = totals[r] * gate
            factor[c, rows] = gate * spread([part[rows] for part in table_parts], 2, c)

    @pl.when(i < 2)
    def _():
        p_in[...] = jnp.zeros_like(p_in)

    p_copies = [
        pltpu.make_async_remote_copy(
            src_ref=p_out.at[j],
            dst_ref=p_in.at[j],
            send_sem=p_s.at[j],
            recv_sem=p_r.at[j],
            device_id=(lax.rem(i + 2, n), hd),
            device_id_type=MESH,
        )
        for j in range(count)
    ]
    e_copies = [
        to_partner(e_send.at[j], e_recv.at[j], e_s.at[j], e_r.at[j]) for j in range(count)
    ]

    early = y == 0
    d_copy.wait_recv()
    queue = list(range(chunks))
    for _ in range(BEFORE):
        inside(queue.pop(0))
    squares = jnp.zeros((span, LANES), jnp.float32)

    def gate_in(c, state, squares):
        gated = within[c] + dot(read_vec, state) * factor[c]
        within[c] = gated
        return squares + gated * gated

    for j in range(half):
        c = y * half + j
        d_mine = d_own[pl.ds(c, 1), :]
        d_other = d_recv[pl.ds(c, 1), :]
        d_first = jnp.where(early, d_mine, d_other)
        d_second = jnp.where(early, d_other, d_mine)
        for r in range(SPLIT):
            k = j * SPLIT + r
            part = slice(r * tall, (r + 1) * tall)
            s_copies[k].wait_recv()
            mine = s_own[j, part]
            other = s_recv[k].astype(jnp.float32)
            first = jnp.where(early, mine, other)
            second = jnp.where(early, other, mine)
            kept = d_second * first + second
            both = d_second * d_first

            @pl.when(has_before)
            def _():
                p_copies[k].wait_recv()

            before = p_in[k].astype(jnp.float32)

            @pl.when(has_after)
            def _():
                p_out[k] = (both * before + kept).astype(jnp.bfloat16)
                p_copies[k].start()

            middle = d_first * before + first
            e_send[k] = jnp.where(early, middle, before).astype(jnp.bfloat16)
            e_copies[k].start()
            e_own[j, part] = jnp.where(early, before, middle).astype(jnp.bfloat16)
        if queue:
            inside(queue.pop(0))
    while queue:
        inside(queue.pop(0))

    for j in range(half):
        squares = gate_in(y * half + j, e_own[j], squares)
    for j in range(half):
        for r in range(SPLIT):
            e_copies[j * SPLIT + r].wait_recv()
        state = jnp.concatenate([e_recv[j * SPLIT + r] for r in range(SPLIT)], axis=0)
        squares = gate_in((1 - y) * half + j, state, squares)

    row = jnp.sum(jnp.transpose(squares), axis=0, keepdims=True)
    sq_send[...] = row
    sq_copies = [
        pltpu.make_async_remote_copy(
            src_ref=sq_send,
            dst_ref=sq_recv.at[k - 1],
            send_sem=sq_s.at[k - 1],
            recv_sem=sq_r.at[k - 1],
            device_id=(i, lax.rem(hd + k, m)),
            device_id_type=MESH,
        )
        for k in range(1, m)
    ]
    for copy in sq_copies:
        copy.start()
    for copy in sq_copies:
        copy.wait_recv()
    for k in range(1, m):
        row = row + sq_recv[k - 1, 0:1]
    scale = lax.rsqrt(row / total_channels + 1.0)
    scale = jnp.transpose(jnp.broadcast_to(scale, (LANES, span)))
    out_copies = []
    for c in range(chunks):
        cols = slice(c * LANES, (c + 1) * LANES)
        out_v[c] = (within[c] * scale * gain_ref[:, cols]).astype(jnp.bfloat16)
        out_copies.append(pltpu.make_async_copy(out_v.at[c], out_ref.at[:, cols], out_sem.at[c]))
        out_copies[c].start()

    @pl.when(has_next)
    def _():
        halo_copy.wait_send()

    d_copy.wait_send()
    for copy in s_copies + e_copies + sq_copies:
        copy.wait_send()

    @pl.when(has_after)
    def _():
        for copy in p_copies:
            copy.wait_send()

    for copy in out_copies:
        copy.wait()


def shards(n, m, x, gate, proj, raw, bias, rate, cf, cp, gain):
    _, span, channels = x.shape
    heads = rate.shape[0]
    chunks = channels // LANES
    state = proj.shape[2] // 2
    half = chunks // 2
    count, tall = half * SPLIT, state // SPLIT
    f32, bf16 = jnp.float32, jnp.bfloat16
    dma = pltpu.SemaphoreType.DMA
    any_spec = pl.BlockSpec(memory_space=pl.ANY)
    vmem = pl.BlockSpec(memory_space=pltpu.VMEM)
    result = pl.pallas_call(
        functools.partial(kernel, n, m, channels * m),
        out_shape=jax.ShapeDtypeStruct((span, channels), bf16),
        in_specs=[any_spec] * 4 + [vmem] * 5,
        out_specs=any_spec,
        scratch_shapes=[
            pltpu.VMEM((chunks, span, LANES), bf16),
            pltpu.VMEM((chunks, span, LANES), bf16),
            pltpu.VMEM((2, span, LANES), bf16),
            pltpu.VMEM((heads, span), f32),
            pltpu.VMEM((8, channels + 2 * state), bf16),
            pltpu.VMEM((8, channels + 2 * state), bf16),
            pltpu.VMEM((chunks, span + 8, LANES), f32),
            pltpu.VMEM((2, span + 8, LANES), f32),
            pltpu.VMEM((chunks, span, LANES), bf16),
            pltpu.VMEM((chunks, span, LANES), f32),
            pltpu.VMEM((chunks, span, LANES), f32),
            pltpu.VMEM((chunks, state, LANES), f32),
            pltpu.VMEM((chunks, span, LANES), bf16),
            pltpu.VMEM((count, tall, LANES), bf16),
            pltpu.VMEM((count, tall, LANES), bf16),
            pltpu.VMEM((half, state, LANES), f32),
            pltpu.VMEM((chunks, LANES), f32),
            pltpu.VMEM((chunks, LANES), f32),
            pltpu.VMEM((count, tall, LANES), bf16),
            pltpu.VMEM((count, tall, LANES), bf16),
            pltpu.VMEM((half, state, LANES), bf16),
            pltpu.VMEM((count, tall, LANES), bf16),
            pltpu.VMEM((count, tall, LANES), bf16),
            pltpu.VMEM((1, span), f32),
            pltpu.VMEM((m - 1, 1, span), f32),
            dma((chunks,)),
            dma((chunks,)),
            dma((5,)),
            dma((chunks,)),
            dma,
            dma,
            dma,
            dma,
            dma((count,)),
            dma((count,)),
            dma((count,)),
            dma((count,)),
            dma((count,)),
            dma((count,)),
            dma((m - 1,)),
            dma((m - 1,)),
        ],
        compiler_params=pltpu.CompilerParams(collective_id=0, has_side_effects=True),
    )(x[0], gate[0], proj[0], jnp.transpose(raw[0]), bias[None], rate[None], cf, cp, gain[None])
    return result[None]


def solution(mesh):
    sizes = mesh.shape
    return jax.shard_map(
        functools.partial(shards, sizes["seq"], sizes["head"]),
        mesh=mesh,
        in_specs=(
            P(None, "seq", "head"),
            P(None, "seq", "head"),
            P(None, "seq", None),
            P(None, "seq", "head"),
            P("head"),
            P("head"),
            P(None, "head"),
            P(),
            P("head"),
        ),
        out_specs=P(None, "seq", "head"),
        check_vma=False,
    )
```

```python
import functools
import math

import jax
import jax.numpy as jnp
from jax import lax
from jax.experimental import pallas as pl
from jax.experimental.pallas import tpu as pltpu
from jax.sharding import PartitionSpec as P

HEADS = 64
HEAD_DIM = 64
STRETCH = 256
LANES = 128
LOG2E = math.log2(math.e)
FIX = 16
SPLIT = 2
BEFORE = 4
MESH = pl.DeviceIdType.MESH


def silu(value):
    half = 0.5 * value
    return half + half * jnp.tanh(half)


def pieces(value, count):
    parts = []
    for _ in range(count):
        part = value.astype(jnp.bfloat16)
        parts.append(part)
        value = value - part.astype(jnp.float32)
    return parts


def dot(a, b):
    return jnp.dot(a, b, preferred_element_type=jnp.float32)


def dot_parts(parts, b):
    total = dot(parts[-1], b)
    for part in parts[-2::-1]:
        total = total + dot(part, b)
    return total


def iota(shape, dim):
    return lax.broadcasted_iota(jnp.int32, shape, dim)


def conv(wide, slot, weights, span):
    taps = weights.shape[0]
    first = 8 - taps + 1
    total = wide[slot, first : first + span] * weights[0:1]
    for k in range(1, taps):
        total = total + wide[slot, first + k : first + k + span] * weights[k : k + 1]
    return silu(total)


def kernel(
    n,
    m,
    total_channels,
    x_hbm,
    gate_hbm,
    proj_hbm,
    raw_hbm,
    bias_ref,
    rate_ref,
    cf_ref,
    cp_ref,
    gain_ref,
    out_ref,
    x_v,
    gate_v,
    proj_v,
    raw_v,
    halo_out,
    halo_in,
    wide_x,
    wide_p,
    xm,
    within,
    factor,
    s_part,
    out_v,
    s_send,
    s_recv,
    s_own,
    d_own,
    d_recv,
    p_in,
    p_out,
    e_own,
    e_send,
    e_recv,
    sq_send,
    sq_recv,
    x_sem,
    gate_sem,
    misc_sem,
    out_sem,
    halo_s,
    halo_r,
    d_s,
    d_r,
    s_s,
    s_r,
    p_s,
    p_r,
    e_s,
    e_r,
    sq_s,
    sq_r,
):
    span = proj_v.shape[1]
    chunks = x_v.shape[0]
    half = chunks // 2
    heads = rate_ref.shape[1]
    per = heads // chunks
    width = LANES // per
    i = lax.axis_index("seq")
    hd = lax.axis_index("head")
    y = lax.rem(i, 2)
    partner = i + 1 - 2 * y
    has_prev, has_next = i > 0, i < n - 1
    has_before, has_after = i >= 2, i < n - 2

    barrier = pltpu.get_barrier_semaphore()
    relations = [(has_prev, i - 1), (has_next, i + 1), (has_before, i - 2), (has_after, i + 2)]
    for here, who in relations:

        @pl.when(here)
        def _():
            pl.semaphore_signal(barrier, inc=1, device_id=(who, hd), device_id_type=MESH)

    for k in range(1, m):
        pl.semaphore_signal(
            barrier, inc=1, device_id=(i, lax.rem(hd + k, m)), device_id_type=MESH
        )

    channels = chunks * LANES
    edge = span - halo_in.shape[0]
    edge_copies = [
        pltpu.make_async_copy(
            x_hbm.at[edge:span], halo_out.at[:, 0:channels], misc_sem.at[3]
        ),
        pltpu.make_async_copy(
            proj_hbm.at[edge:span], halo_out.at[:, channels:], misc_sem.at[4]
        ),
    ]
    raw_copy = pltpu.make_async_copy(raw_hbm, raw_v, misc_sem.at[0])
    proj_copies = [
        pltpu.make_async_copy(
            proj_hbm.at[:, k * LANES : (k + 1) * LANES], proj_v.at[k], misc_sem.at[1 + k]
        )
        for k in range(2)
    ]
    for copy in edge_copies + [raw_copy] + proj_copies:
        copy.start()
    x_copies = []
    gate_copies = []
    for c in range(chunks):
        cols = slice(c * LANES, (c + 1) * LANES)
        x_copies.append(pltpu.make_async_copy(x_hbm.at[:, cols], x_v.at[c], x_sem.at[c]))
        gate_copies.append(
            pltpu.make_async_copy(gate_hbm.at[:, cols], gate_v.at[c], gate_sem.at[c])
        )
    for copy in x_copies + gate_copies:
        copy.start()
    def column(row):
        eye = iota((heads, heads), 0) == iota((heads, heads), 1)
        wide = jnp.broadcast_to(row, (heads, heads))
        return jnp.sum(jnp.where(eye, wide, 0.0), axis=1, keepdims=True)

    raw_copy.wait()
    shifted = raw_v[...] + column(bias_ref[...])
    step = jnp.maximum(shifted, 0.0) + jnp.log1p(jnp.exp(-jnp.abs(shifted)))
    upto = (iota((span, span), 0) <= iota((span, span), 1)).astype(jnp.bfloat16)
    lead = (step * (-LOG2E)) * column(rate_ref[...])
    run_t = dot_parts(pieces(lead, 3), upto)
    source_t = run_t - LOG2E * jnp.log(step)
    last = run_t[:, span - 1 : span]
    to_end = jnp.exp2(last - source_t)
    token = iota((heads, span), 1)
    rows = [
        run_t,
        jnp.where(token < FIX, 0.0, to_end),
        jnp.exp2(run_t),
        jnp.where(token < FIX, to_end, 0.0),
    ]
    rows.append(jnp.zeros((LANES - len(rows) * heads, span), jnp.float32))
    table = jnp.transpose(jnp.concatenate(rows, axis=0))
    run = table

    def spread(kind, c, rows):
        first = kind * heads + c * per
        size = rows.stop - rows.start
        lane = iota((size, LANES), 1) // width
        result = jnp.broadcast_to(table[rows, first : first + 1], (size, LANES))
        for q in range(1, per):
            result = jnp.where(lane == q, table[rows, first + q : first + q + 1], result)
        return result

    lane_of = iota((heads, LANES), 0) % per == iota((heads, LANES), 1) // width
    ends = jnp.where(lane_of, jnp.exp2(last), 0.0)
    owner = (iota((chunks, heads), 1) // per == iota((chunks, heads), 0)).astype(jnp.bfloat16)
    ends_parts = pieces(ends, 3)
    d_own[...] = dot(owner, ends_parts[2]) + dot(owner, ends_parts[1]) + dot(owner, ends_parts[0])

    def to_partner(src, dst, send_sem, recv_sem):
        return pltpu.make_async_remote_copy(
            src_ref=src,
            dst_ref=dst,
            send_sem=send_sem,
            recv_sem=recv_sem,
            device_id=(partner, hd),
            device_id_type=MESH,
        )

    d_copy = to_partner(d_own, d_recv, d_s, d_r)
    for copy in edge_copies:
        copy.wait()

    pl.semaphore_wait(barrier, sum(here.astype(jnp.int32) for here, _ in relations) + m - 1)

    halo_copy = pltpu.make_async_remote_copy(
        src_ref=halo_out,
        dst_ref=halo_in,
        send_sem=halo_s,
        recv_sem=halo_r,
        device_id=(lax.rem(i + 1, n), hd),
        device_id_type=MESH,
    )

    @pl.when(has_next)
    def _():
        halo_copy.start()

    d_copy.start()

    for copy in proj_copies:
        copy.wait()
    mixed = []
    for k in range(2):
        cols = slice(k * LANES, (k + 1) * LANES)
        wide_p[k, 0:8] = jnp.zeros((8, LANES), jnp.float32)
        wide_p[k, 8 : 8 + span] = proj_v[k].astype(jnp.float32)
        mixed.append(conv(wide_p, k, cp_ref[:, cols], span))
    write_t = jnp.transpose(mixed[0])
    write_main = write_t.astype(jnp.bfloat16)

    for c in range(chunks):
        x_copies[c].wait()
        wide_x[c, 0:8] = jnp.zeros((8, LANES), jnp.float32)
        wide_x[c, 8 : 8 + span] = x_v[c].astype(jnp.float32)
        x_c = conv(wide_x, c, cf_ref[:, c * LANES : (c + 1) * LANES], span)
        x_c = x_c.astype(jnp.bfloat16)
        xm[c] = x_c
        weighted = x_c.astype(jnp.float32) * spread(1, c, slice(0, span))
        s_part[c] = dot(write_main, weighted.astype(jnp.bfloat16))

    @pl.when(has_prev)
    def _():
        halo_copy.wait_recv()

    @pl.when(i == 0)
    def _():
        halo_in[...] = jnp.zeros_like(halo_in)

    fixed = []
    for k in range(2):
        cols = slice(k * LANES, (k + 1) * LANES)
        lanes = slice(channels + k * LANES, channels + (k + 1) * LANES)
        wide_p[k, 0:8] = halo_in[:, lanes].astype(jnp.float32)
        fixed.append(conv(wide_p, k, cp_ref[:, cols], FIX))
    blank = jnp.zeros((LANES - FIX, LANES), jnp.float32)
    fix_t = jnp.transpose(jnp.concatenate([fixed[0], blank], axis=0))
    fix_write = fix_t[:, 0:FIX].astype(jnp.bfloat16)

    count = half * SPLIT
    tall = s_recv.shape[1]
    for c in range(chunks):
        cols = slice(c * LANES, (c + 1) * LANES)
        wide_x[c, 0:8] = halo_in[:, cols].astype(jnp.float32)
        x_c = conv(wide_x, c, cf_ref[:, cols], FIX).astype(jnp.bfloat16)
        xm[c, 0:FIX] = x_c
        weighted = x_c.astype(jnp.float32) * spread(3, c, slice(0, FIX))
        whole = s_part[c] + dot(fix_write, weighted.astype(jnp.bfloat16))
        s_own[c] = whole
        for r in range(SPLIT):
            s_send[c * SPLIT + r] = whole[r * tall : (r + 1) * tall].astype(jnp.bfloat16)
    s_copies = [
        to_partner(s_send.at[(1 - y) * count + j], s_recv.at[j], s_s.at[j], s_r.at[j])
        for j in range(count)
    ]
    for copy in s_copies:
        copy.start()

    head_t = jnp.where(iota((LANES, LANES), 1) < FIX, fix_t, write_t[:, 0:LANES])
    write_t = jnp.concatenate([head_t, write_t[:, LANES:]], axis=1).astype(jnp.bfloat16)
    read_vec = jnp.concatenate([fixed[1], mixed[1][FIX:]], axis=0).astype(jnp.bfloat16)
    scores = dot(read_vec, write_t)
    side = LANES
    steps_in = span // side
    causal = iota((side, side), 0) >= iota((side, side), 1)
    low = iota((span, LANES), 1) // width

    def inside(c):
        x_c = xm[c]
        totals = [None] * steps_in
        for q in range(per):
            h = c * per + q
            x_q = jnp.where(low == q, x_c.astype(jnp.float32), 0.0).astype(jnp.bfloat16)
            for r in range(steps_in):
                rows = slice(r * side, (r + 1) * side)
                now = run[rows, h : h + 1]
                tiles = []
                for k in range(r + 1):
                    cols = slice(k * side, (k + 1) * side)
                    gap = now - source_t[h : h + 1, cols]
                    if k == r:
                        gap = jnp.where(causal, gap, -1e30)
                    tiles.append((scores[rows, cols] * jnp.exp2(gap)).astype(jnp.bfloat16))
                mixing = tiles[0] if r == 0 else jnp.concatenate(tiles, axis=1)
                term = dot(mixing, x_q[0 : (r + 1) * side])
                totals[r] = term if totals[r] is None else totals[r] + term
        gate_copies[c].wait()
        for r in range(steps_in):
            rows = slice(r * side, (r + 1) * side)
            gate = silu(gate_v[c, rows].astype(jnp.float32))
            within[c, rows] = totals[r] * gate
            factor[c, rows] = gate * spread(2, c, rows)

    @pl.when(i < 2)
    def _():
        p_in[...] = jnp.zeros_like(p_in)

    p_copies = [
        pltpu.make_async_remote_copy(
            src_ref=p_out.at[j],
            dst_ref=p_in.at[j],
            send_sem=p_s.at[j],
            recv_sem=p_r.at[j],
            device_id=(lax.rem(i + 2, n), hd),
            device_id_type=MESH,
        )
        for j in range(count)
    ]
    e_copies = [
        to_partner(e_send.at[j], e_recv.at[j], e_s.at[j], e_r.at[j]) for j in range(count)
    ]

    early = y == 0
    d_copy.wait_recv()
    queue = list(range(chunks))
    for _ in range(BEFORE):
        inside(queue.pop(0))
    squares = jnp.zeros((span, LANES), jnp.float32)

    def gate_in(c, state, squares):
        gated = within[c] + dot(read_vec, state) * factor[c]
        wide_x[c, 8 : 8 + span] = gated
        return squares + gated * gated

    for j in range(half):
        c = y * half + j
        d_mine = d_own[pl.ds(c, 1), :]
        d_other = d_recv[pl.ds(c, 1), :]
        d_first = jnp.where(early, d_mine, d_other)
        d_second = jnp.where(early, d_other, d_mine)
        for r in range(SPLIT):
            k = j * SPLIT + r
            part = slice(r * tall, (r + 1) * tall)
            s_copies[k].wait_recv()
            mine = s_own[c, part]
            other = s_recv[k].astype(jnp.float32)
            first = jnp.where(early, mine, other)
            second = jnp.where(early, other, mine)
            kept = d_second * first + second
            both = d_second * d_first

            @pl.when(has_before)
            def _():
                p_copies[k].wait_recv()

            before = p_in[k].astype(jnp.float32)

            @pl.when(has_after)
            def _():
                p_out[k] = (both * before + kept).astype(jnp.bfloat16)
                p_copies[k].start()

            middle = d_first * before + first
            e_send[k] = jnp.where(early, middle, before).astype(jnp.bfloat16)
            e_copies[k].start()
            e_own[j, part] = jnp.where(early, before, middle).astype(jnp.bfloat16)
        if queue:
            inside(queue.pop(0))
    while queue:
        inside(queue.pop(0))

    for j in range(half):
        squares = gate_in(y * half + j, e_own[j], squares)
    for j in range(half):
        for r in range(SPLIT):
            e_copies[j * SPLIT + r].wait_recv()
        state = jnp.concatenate([e_recv[j * SPLIT + r] for r in range(SPLIT)], axis=0)
        squares = gate_in((1 - y) * half + j, state, squares)

    row = jnp.sum(jnp.transpose(squares), axis=0, keepdims=True)
    sq_send[...] = row
    sq_copies = [
        pltpu.make_async_remote_copy(
            src_ref=sq_send,
            dst_ref=sq_recv.at[k - 1],
            send_sem=sq_s.at[k - 1],
            recv_sem=sq_r.at[k - 1],
            device_id=(i, lax.rem(hd + k, m)),
            device_id_type=MESH,
        )
        for k in range(1, m)
    ]
    for copy in sq_copies:
        copy.start()
    for copy in sq_copies:
        copy.wait_recv()
    for k in range(1, m):
        row = row + sq_recv[k - 1, 0:1]
    scale = lax.rsqrt(row / total_channels + 1.0)
    scale = jnp.transpose(jnp.broadcast_to(scale, (LANES, span)))
    out_copies = []
    for c in range(chunks):
        cols = slice(c * LANES, (c + 1) * LANES)
        out_v[c] = (wide_x[c, 8 : 8 + span] * scale * gain_ref[:, cols]).astype(jnp.bfloat16)
        out_copies.append(pltpu.make_async_copy(out_v.at[c], out_ref.at[:, cols], out_sem.at[c]))
        out_copies[c].start()

    @pl.when(has_next)
    def _():
        halo_copy.wait_send()

    d_copy.wait_send()
    for copy in s_copies + e_copies + sq_copies:
        copy.wait_send()

    @pl.when(has_after)
    def _():
        for copy in p_copies:
            copy.wait_send()

    for copy in out_copies:
        copy.wait()


def shards(n, m, x, gate, proj, raw, bias, rate, cf, cp, gain):
    _, span, channels = x.shape
    heads = rate.shape[0]
    chunks = channels // LANES
    state = proj.shape[2] // 2
    half = chunks // 2
    count, tall = half * SPLIT, state // SPLIT
    f32, bf16 = jnp.float32, jnp.bfloat16
    dma = pltpu.SemaphoreType.DMA
    any_spec = pl.BlockSpec(memory_space=pl.ANY)
    vmem = pl.BlockSpec(memory_space=pltpu.VMEM)
    result = pl.pallas_call(
        functools.partial(kernel, n, m, channels * m),
        out_shape=jax.ShapeDtypeStruct((span, channels), bf16),
        in_specs=[any_spec] * 4 + [vmem] * 5,
        out_specs=any_spec,
        scratch_shapes=[
            pltpu.VMEM((chunks, span, LANES), bf16),
            pltpu.VMEM((chunks, span, LANES), bf16),
            pltpu.VMEM((2, span, LANES), bf16),
            pltpu.VMEM((heads, span), f32),
            pltpu.VMEM((8, channels + 2 * state), bf16),
            pltpu.VMEM((8, channels + 2 * state), bf16),
            pltpu.VMEM((chunks, span + 8, LANES), f32),
            pltpu.VMEM((2, span + 8, LANES), f32),
            pltpu.VMEM((chunks, span, LANES), bf16),
            pltpu.VMEM((chunks, span, LANES), f32),
            pltpu.VMEM((chunks, span, LANES), f32),
            pltpu.VMEM((chunks, state, LANES), f32),
            pltpu.VMEM((chunks, span, LANES), bf16),
            pltpu.VMEM((2 * count, tall, LANES), bf16),
            pltpu.VMEM((count, tall, LANES), bf16),
            pltpu.VMEM((chunks, state, LANES), f32),
            pltpu.VMEM((chunks, LANES), f32),
            pltpu.VMEM((chunks, LANES), f32),
            pltpu.VMEM((count, tall, LANES), bf16),
            pltpu.VMEM((count, tall, LANES), bf16),
            pltpu.VMEM((half, state, LANES), bf16),
            pltpu.VMEM((count, tall, LANES), bf16),
            pltpu.VMEM((count, tall, LANES), bf16),
            pltpu.VMEM((1, span), f32),
            pltpu.VMEM((m - 1, 1, span), f32),
            dma((chunks,)),
            dma((chunks,)),
            dma((5,)),
            dma((chunks,)),
            dma,
            dma,
            dma,
            dma,
            dma((count,)),
            dma((count,)),
            dma((count,)),
            dma((count,)),
            dma((count,)),
            dma((count,)),
            dma((m - 1,)),
            dma((m - 1,)),
        ],
        compiler_params=pltpu.CompilerParams(collective_id=0, has_side_effects=True),
    )(x[0], gate[0], proj[0], jnp.transpose(raw[0]), bias[None], rate[None], cf, cp, gain[None])
    return result[None]


def solution(mesh):
    sizes = mesh.shape
    return jax.shard_map(
        functools.partial(shards, sizes["seq"], sizes["head"]),
        mesh=mesh,
        in_specs=(
            P(None, "seq", "head"),
            P(None, "seq", "head"),
            P(None, "seq", None),
            P(None, "seq", "head"),
            P("head"),
            P("head"),
            P(None, "head"),
            P(),
            P("head"),
        ),
        out_specs=P(None, "seq", "head"),
        check_vma=False,
    )
```
